32 devices in a mesh: node: 8 (over z, x), local: 4 (over y, core).
Axes of the slice: x: 2, y: 2, z: 4, core: 2. Of those that a mesh axis runs over, the one named last changes fastest.
Arguments:
- tokens: bfloat16 [128, 3584], P(('node', 'local')), may hold values from -6 to 6
- expert_ids: int32 [128, 6], P(('node', 'local')), may hold values from 0 to 15, as said below
- gate_codes: int32 [128, 6], P(('node', 'local')), may hold values from 1 to 1023
- gate_proj: bfloat16 [3584, 16384], P(None, ('node', 'local')), may hold values from -0.09375 to 0.09375
- up_proj: bfloat16 [3584, 16384], P(None, ('node', 'local')), may hold values from -0.09375 to 0.09375
- down_proj: bfloat16 [16384, 3584], P('node', 'local'), may hold values from -0.1875 to 0.1875
Outputs:
- routed: bfloat16 [128, 3584], P(('node', 'local'))
The draws below stay inside these ranges and needn't reach their ends.
Inputs may be any that keep to these rules, and one draw needn't show every extreme that they name: `expert_ids`: each token names 6 different experts, lying in exactly 4 node groups with at least one named expert in each. The tokens of one device name each node group at most 2 times in all and some node group exactly 2 times; where 8 divides 4 * 4, they name every node group exactly 2 times. For every local index, the tokens of all devices with that local index together name each node group exactly 4 * 4 times.
All inputs are finite; a program needn't handle non-finite values.
Results may differ from the reference program's by a relative error of at most 0.02.
Values may be sent and summed in bfloat16 or wider, within the bound.
No kernel may reach another device: no remote copies, remote signals or barrier semaphores. Data moves between devices by JAX's collectives and lax.ppermute only.
A program may use at most 64 MiB of HBM per device.

```python
import jax
import jax.numpy as jnp
from jax import lax

D = 3584
FF_E = 1024
EXP_NODE = 2
NL = 4
TOP = 6
TOK_DEV = 4
EXPERTS = 16
TOKENS = 128
N_NODE = 8
N_LOCAL = 4


def draw_expert_ids(key, part):
    key_offset, key_mapping, key_drop = jax.random.split(key, 3)
    offsets = jax.vmap(lambda single: jax.random.permutation(single, N_NODE))(jax.random.split(key_offset, N_LOCAL))
    mapping = jax.vmap(lambda single: jax.random.permutation(single, N_NODE))(jax.random.split(key_mapping, N_LOCAL))
    node_index = jnp.arange(N_NODE, dtype=jnp.int32)[:, None, None, None]
    lane_index = jnp.arange(N_LOCAL, dtype=jnp.int32)[None, :, None, None]
    choice_index = jnp.arange(TOK_DEV, dtype=jnp.int32)[None, None, :, None] * NL + jnp.arange(NL, dtype=jnp.int32)[None, None, None, :]
    shifted = offsets[lane_index, choice_index % N_NODE]
    target = mapping[lane_index, (node_index + shifted) % N_NODE]
    shape = (N_NODE, N_LOCAL, TOK_DEV)
    key_first, key_second, key_side = jax.random.split(key_drop, 3)
    first = jax.random.randint(key_first, shape, 0, NL)
    second = (first + jax.random.randint(key_second, shape, 1, NL)) % NL
    sides = jax.random.randint(key_side, shape + (2,), 0, EXP_NODE)
    candidates = target[..., None] * EXP_NODE + jnp.arange(EXP_NODE, dtype=jnp.int32)
    slot_k = jnp.arange(NL, dtype=jnp.int32)[:, None]
    slot_e = jnp.arange(EXP_NODE, dtype=jnp.int32)[None, :]
    dropped = (slot_k == first[..., None, None]) & (slot_e == sides[..., 0, None, None]) | (slot_k == second[..., None, None]) & (slot_e == sides[..., 1, None, None])
    flat_cand = candidates.reshape(shape + (NL * EXP_NODE,))
    flat_drop = dropped.reshape(shape + (NL * EXP_NODE,)).astype(jnp.int32)
    keyed = flat_drop * (NL * EXP_NODE) + jnp.arange(NL * EXP_NODE, dtype=jnp.int32)
    kept = jnp.argsort(keyed, axis=-1)[..., :TOP]
    picked = jnp.take_along_axis(flat_cand, kept, axis=-1)
    return picked.reshape(N_NODE * N_LOCAL * TOK_DEV, TOP).astype(jnp.int32)


def touch_ends(result, own_key, least, largest):
    extent = result.shape
    spot = [jax.random.randint(jax.random.fold_in(own_key, axis), (), 0, extent[axis]) for axis in range(len(extent))]
    result = result.at[tuple(spot)].set(least)
    longest = extent.index(max(extent))
    spot[longest] = (spot[longest] + 1) % extent[longest]
    return result.at[tuple(spot)].set(largest)


def steps_of(stream_key, shape, shards, low, largest):
    loudness = 1.0
    for axis_at, blocks in shards:
        draws = jax.random.uniform(jax.random.fold_in(jax.random.fold_in(stream_key, 6), axis_at), (blocks,), jnp.float32, low / len(shards), largest / len(shards))
        loudness = loudness * jnp.repeat(jnp.exp(draws), shape[axis_at] // blocks).reshape((-1,) + (1,) * (len(shape) - 1 - axis_at))
    return loudness


def normal_values(rng, shape, deviation, reach, pieces=(), kind=jnp.bfloat16):
    level = steps_of(rng, shape, pieces, -0.22, 0.18) if pieces else 1.0
    array = jax.random.normal(rng, shape, jnp.float32) * deviation * level
    return jnp.minimum(jnp.maximum(array, -reach), reach).astype(kind)


def setup_inputs(seed: int = 0) -> dict:
    splits = jax.random.split(jax.random.key(seed), 7)
    return {
        "tokens": normal_values(splits[0], (TOKENS, D), 1.0, 6.0, ((0, 32),)),
        "expert_ids": draw_expert_ids(jax.random.fold_in(splits[6], 71), 0),
        "gate_codes": touch_ends(jax.random.randint(splits[2], (TOKENS, TOP), 1, 1024), jax.random.fold_in(splits[2], 1), 1, 1023).astype(jnp.int32),
        "gate_proj": normal_values(splits[3], (D, EXPERTS * FF_E), D ** -0.5, 0.09375, ((1, 32),)),
        "up_proj": normal_values(splits[4], (D, EXPERTS * FF_E), D ** -0.5, 0.09375, ((1, 32),)),
        "down_proj": normal_values(splits[5], (EXPERTS * FF_E, D), FF_E ** -0.5, 0.1875, ((0, 8), (1, 4))),
    }


ROUTE_SCALE = 2.5


def reference(tokens, expert_ids, gate_codes, gate_proj, up_proj, down_proj):
    codes_float = gate_codes.astype(jnp.float32)
    weights = ROUTE_SCALE * codes_float / jnp.sum(codes_float, axis=1, keepdims=True)
    node_of = expert_ids // EXP_NODE
    expert_side = expert_ids % EXP_NODE
    node_rows = N_LOCAL * TOK_DEV * NL
    node_width = EXP_NODE * FF_E

    def one_group(summed, node_group):
        node_hit = node_of == node_group
        node_used = jnp.any(node_hit, axis=1).astype(jnp.int32)
        picked = jnp.argsort(1 - node_used, stable=True)[:node_rows].astype(jnp.int32)
        chosen = jnp.take(tokens, picked, axis=0)
        gate_pair = jnp.stack(
            [jnp.sum(jnp.where(node_hit & (expert_side == side_index), weights, 0.0), axis=1)
             for side_index in range(EXP_NODE)], axis=1)
        gate_pair = jnp.take(gate_pair, picked, axis=0)
        start_col = (node_group * node_width).astype(jnp.int32)
        gate_block = lax.dynamic_slice_in_dim(gate_proj, start_col, node_width, 1)
        up_block = lax.dynamic_slice_in_dim(up_proj, start_col, node_width, 1)
        down_block = lax.dynamic_slice_in_dim(down_proj, start_col, node_width, 0)
        pre_gate = jnp.dot(chosen, gate_block, preferred_element_type=jnp.float32)
        pre_up = jnp.dot(chosen, up_block, preferred_element_type=jnp.float32)
        gate_scale = jnp.repeat(gate_pair, FF_E, axis=1)
        hidden = (gate_scale * jax.nn.silu(pre_gate) * pre_up).astype(jnp.bfloat16)
        contrib = jnp.dot(hidden, down_block, preferred_element_type=jnp.float32).astype(jnp.bfloat16)
        summed = summed.at[picked].add(contrib.astype(jnp.float32))
        return summed, None

    summed, ignored = lax.scan(one_group, jnp.zeros(tokens.shape, jnp.float32),
                               jnp.arange(N_NODE, dtype=jnp.int32))
    return summed.astype(jnp.bfloat16)
```

```python
import functools

import jax
import jax.numpy as jnp
from jax import lax
from jax.experimental import pallas as pl
from jax.experimental.pallas import tpu as pltpu
from jax.sharding import PartitionSpec as P

FF_E = 1024
EXP_NODE = 2
NL = 4
ROUTE_SCALE = 2.5
LANES = 128
EVERY = ("node", "local")


def slot_mask(ids, group, slot):
    rows = ids.shape[0]
    node_of = ids // EXP_NODE
    used = jnp.zeros(group.shape, jnp.bool_)
    for k in range(ids.shape[1]):
        used = used | (node_of[:, k : k + 1] == group)
    used = used.astype(jnp.int32)
    ranks, so_far = [], jnp.zeros((1, group.shape[1]), jnp.int32)
    for t in range(rows):
        ranks.append(so_far)
        so_far = so_far + used[t : t + 1]
    rank = jnp.concatenate(ranks, axis=0)
    return jnp.where((used > 0) & (rank == slot), 1.0, 0.0)


def dispatch_kernel(nodes, lanes_local, slots, tok_ref, ids_ref, codes_ref, out_ref):
    ids = ids_ref[...]
    rows, top = ids.shape
    width = tok_ref.shape[1]
    half = width // 2
    codes = codes_ref[...].astype(jnp.float32)
    weight = ROUTE_SCALE * codes / jnp.sum(codes, axis=1, keepdims=True)
    high = weight.astype(jnp.bfloat16).astype(jnp.float32)
    middle = (weight - high).astype(jnp.bfloat16).astype(jnp.float32)
    low = weight - high - middle
    lane = lax.broadcasted_iota(jnp.int32, (rows, LANES), 1)
    score = jnp.zeros((rows, LANES), jnp.float32)
    for part, values in enumerate((ids.astype(jnp.float32), high, middle, low)):
        for k in range(top):
            score = jnp.where(lane == part * top + k, values[:, k : k + 1], score)
    count = nodes * slots
    spot = lax.broadcasted_iota(jnp.int32, (rows, count), 1)
    mask = slot_mask(ids, spot // slots, spot % slots).astype(jnp.bfloat16)
    contract = (((0,), (0,)), ((), ()))
    placed = lax.dot_general(mask, tok_ref[...], contract, preferred_element_type=jnp.float32).astype(jnp.bfloat16)
    scored = lax.dot_general(
        mask, score.astype(jnp.bfloat16), contract, preferred_element_type=jnp.float32
    ).astype(jnp.bfloat16)
    for n in range(nodes):
        own = slice(n * slots, (n + 1) * slots)
        for l in range(lanes_local):
            side = l % 2
            out_ref[n * lanes_local + l, :, :half] = placed[own, side * half : (side + 1) * half]
            out_ref[n * lanes_local + l, :, half:] = scored[own]


def combine_kernel(nodes, lanes_local, slots, ids_ref, back_ref, out_ref):
    ids = ids_ref[...]
    rows = ids.shape[0]
    piece = back_ref.shape[1]
    count = nodes * lanes_local * slots
    spot = lax.broadcasted_iota(jnp.int32, (rows, count), 1)
    mask = slot_mask(ids, spot // (lanes_local * slots), spot % slots)
    owner = (spot // slots) % lanes_local
    pick = jnp.concatenate([jnp.where(owner == l, mask, 0.0) for l in range(lanes_local)], axis=0)
    summed = jnp.dot(pick.astype(jnp.bfloat16), back_ref[...], preferred_element_type=jnp.float32)
    for l in range(lanes_local):
        out_ref[:, l * piece : (l + 1) * piece] = summed[l * rows : (l + 1) * rows].astype(jnp.bfloat16)


def on_device(tokens, expert_ids, gate_codes, gate_proj, up_proj, down_proj):
    nodes, locals_ = lax.axis_size("node"), lax.axis_size("local")
    own_rows, width = tokens.shape
    slots = -(-(own_rows * NL) // nodes)
    devices = nodes * locals_
    half = width // 2
    send = pl.pallas_call(
        functools.partial(dispatch_kernel, nodes, locals_, slots),
        out_shape=jax.ShapeDtypeStruct((devices, slots, half + LANES), jnp.bfloat16),
        name="dispatch",
    )(tokens, expert_ids, gate_codes)
    arrived = lax.all_to_all(send, EVERY, split_axis=0, concat_axis=0, tiled=True)
    arrived = arrived.reshape(devices * slots, half + LANES)
    mine, score = arrived[:, :half], arrived[:, half:].astype(jnp.float32)
    other = lax.ppermute(mine, "local", [(i, i ^ 1) for i in range(locals_)])
    local = lax.axis_index("local")
    chosen = jnp.where(
        local % 2 == 0,
        jnp.concatenate([mine, other], axis=1),
        jnp.concatenate([other, mine], axis=1),
    )
    per_lane = gate_proj.shape[1]
    expert = lax.axis_index("node") * EXP_NODE + local * per_lane // FF_E
    top = expert_ids.shape[1]
    named = score[:, :top] == expert.astype(jnp.float32)
    weight = score[:, top : 2 * top] + score[:, 2 * top : 3 * top] + score[:, 3 * top : 4 * top]
    gate = jnp.sum(jnp.where(named, weight, 0.0), axis=1, keepdims=True)
    pre_gate = jnp.dot(chosen, gate_proj, preferred_element_type=jnp.float32)
    pre_up = jnp.dot(chosen, up_proj, preferred_element_type=jnp.float32)
    hidden = (gate * jax.nn.silu(pre_gate) * pre_up).astype(jnp.bfloat16)
    hidden = lax.all_gather(hidden, "local", axis=1, tiled=True)
    contrib = jnp.dot(hidden, down_proj, preferred_element_type=jnp.float32).astype(jnp.bfloat16)
    back = lax.all_to_all(
        contrib.reshape(devices, slots, -1), EVERY, split_axis=0, concat_axis=0, tiled=True
    ).reshape(devices * slots, -1)
    return pl.pallas_call(
        functools.partial(combine_kernel, nodes, locals_, slots),
        out_shape=jax.ShapeDtypeStruct((own_rows, width), jnp.bfloat16),
        name="combine",
    )(expert_ids, back)


def solution(mesh):
    return jax.shard_map(
        on_device,
        mesh=mesh,
        in_specs=(
            P(EVERY, None),
            P(EVERY, None),
            P(EVERY, None),
            P(None, EVERY),
            P(None, EVERY),
            P("node", "local"),
        ),
        out_specs=P(EVERY, None),
        check_vma=False,
    )
```

```python
import functools

import jax
import jax.numpy as jnp
from jax import lax
from jax.experimental import pallas as pl
from jax.experimental.pallas import tpu as pltpu
from jax.sharding import PartitionSpec as P

FF_E = 1024
EXP_NODE = 2
NL = 4
ROUTE_SCALE = 2.5
LANES = 128
EVERY = ("node", "local")
ANY = pl.BlockSpec(memory_space=pltpu.HBM)
VMEM = pl.BlockSpec(memory_space=pltpu.VMEM)


def small(kib):
    return pltpu.CompilerParams(vmem_limit_bytes=kib << 10)


def resident(array):
    return pltpu.with_memory_space_constraint(array, pltpu.VMEM)


def slot_mask(ids, group, slot):
    rows = ids.shape[0]
    node_of = ids // EXP_NODE
    used = jnp.zeros(group.shape, jnp.bool_)
    for k in range(ids.shape[1]):
        used = used | (node_of[:, k : k + 1] == group)
    used = used.astype(jnp.int32)
    ranks, so_far = [], jnp.zeros((1, group.shape[1]), jnp.int32)
    for t in range(rows):
        ranks.append(so_far)
        so_far = so_far + used[t : t + 1]
    rank = jnp.concatenate(ranks, axis=0)
    return jnp.where((used > 0) & (rank == slot), 1.0, 0.0)


def dispatch_kernel(nodes, lanes_local, slots, tok_hbm, ids_hbm, codes_hbm, out_ref, pick_ref, tok_ref, ids_ref, codes_ref, sems):
    copies = [
        pltpu.make_async_copy(source, target, sems.at[i])
        for i, (source, target) in enumerate(((ids_hbm, ids_ref), (codes_hbm, codes_ref), (tok_hbm, tok_ref)))
    ]
    for copy in copies:
        copy.start()
    copies[0].wait()
    ids = ids_ref[...]
    rows, top = ids.shape
    width = tok_ref.shape[1]
    half = width // 2
    count = nodes * slots
    spot = lax.broadcasted_iota(jnp.int32, (rows, count), 1)
    mask = slot_mask(ids, spot // slots, spot % slots).astype(jnp.bfloat16)
    wide = nodes * lanes_local * slots
    spot = lax.broadcasted_iota(jnp.int32, (rows, wide), 1)
    wide_mask = slot_mask(ids, spot // (lanes_local * slots), spot % slots)
    owner = (spot // slots) % lanes_local
    pick = [jnp.where(owner == l, wide_mask, 0.0) for l in range(lanes_local)]
    pick_ref[...] = jnp.concatenate(pick, axis=0).astype(jnp.bfloat16)
    copies[1].wait()
    codes = codes_ref[...].astype(jnp.float32)
    weight = ROUTE_SCALE * codes / jnp.sum(codes, axis=1, keepdims=True)
    high = weight.astype(jnp.bfloat16).astype(jnp.float32)
    middle = (weight - high).astype(jnp.bfloat16).astype(jnp.float32)
    low = weight - high - middle
    lane = lax.broadcasted_iota(jnp.int32, (rows, LANES), 1)
    score = jnp.zeros((rows, LANES), jnp.float32)
    for part, values in enumerate((ids.astype(jnp.float32), high, middle, low)):
        for k in range(top):
            score = jnp.where(lane == part * top + k, values[:, k : k + 1], score)
    contract = (((0,), (0,)), ((), ()))
    scored = lax.dot_general(
        mask, score.astype(jnp.bfloat16), contract, preferred_element_type=jnp.float32
    ).astype(jnp.bfloat16)
    copies[2].wait()
    placed = lax.dot_general(mask, tok_ref[...], contract, preferred_element_type=jnp.float32).astype(jnp.bfloat16)
    for n in range(nodes):
        own = slice(n * slots, (n + 1) * slots)
        for l in range(lanes_local):
            side = l % 2
            out_ref[n * lanes_local + l, :, :half] = placed[own, side * half : (side + 1) * half]
            out_ref[n * lanes_local + l, :, half:] = scored[own]


def first_kernel(half, mine_ref, gate_ref, up_ref, sum_ref):
    side = lax.axis_index("local") % 2
    part = pl.ds(pl.multiple_of(side * half, half), half)
    width = gate_ref.shape[1]
    mine = mine_ref[:, :, :half].reshape(sum_ref.shape[0], half)
    sum_ref[:, :width] = jnp.dot(mine, gate_ref[part, :], preferred_element_type=jnp.float32)
    sum_ref[:, width:] = jnp.dot(mine, up_ref[part, :], preferred_element_type=jnp.float32)


def second_kernel(half, top, sum_ref, mine_ref, other_ref, gate_ref, up_ref, hidden_ref):
    local = lax.axis_index("local")
    side = 1 - local % 2
    part = pl.ds(pl.multiple_of(side * half, half), half)
    width = gate_ref.shape[1]
    expert = lax.axis_index("node") * EXP_NODE + local * width // FF_E
    rows = sum_ref.shape[0]
    score = mine_ref[:, :, half:].reshape(rows, LANES).astype(jnp.float32)
    named = score[:, :top] == expert.astype(jnp.float32)
    weight = score[:, top : 2 * top] + score[:, 2 * top : 3 * top] + score[:, 3 * top : 4 * top]
    scale = jnp.sum(jnp.where(named, weight, 0.0), axis=1, keepdims=True)
    other = other_ref[:, :, :half].reshape(rows, half)
    pre_gate = sum_ref[:, :width] + jnp.dot(other, gate_ref[part, :], preferred_element_type=jnp.float32)
    pre_up = sum_ref[:, width:] + jnp.dot(other, up_ref[part, :], preferred_element_type=jnp.float32)
    hidden_ref[...] = (scale * (pre_gate / (1.0 + jnp.exp(-pre_gate))) * pre_up).astype(jnp.bfloat16)


def down_near_kernel(mask, *refs):
    count = len(mask)
    pieces, down_ref, sum_ref = refs[:count], refs[count], refs[count + 1]
    local = lax.axis_index("local")
    total = None
    for flip, piece in zip(mask, pieces):
        depth = piece.shape[1]
        part = pl.ds(pl.multiple_of((local ^ flip) * depth, depth), depth)
        term = jnp.dot(piece[...], down_ref[part, :], preferred_element_type=jnp.float32)
        total = term if total is None else total + term
    sum_ref[...] = total


def down_far_kernel(mask, *refs):
    count = len(mask)
    pieces, down_ref, near_ref, out_ref = refs[:count], refs[count], refs[count + 1], refs[count + 2]
    local = lax.axis_index("local")
    total = near_ref[...]
    for flip, piece in zip(mask, pieces):
        depth = piece.shape[1]
        part = pl.ds(pl.multiple_of((local ^ flip) * depth, depth), depth)
        total = total + jnp.dot(piece[...], down_ref[part, :], preferred_element_type=jnp.float32)
    out_ref[...] = total.astype(jnp.bfloat16).reshape(out_ref.shape)


def combine_kernel(lanes_local, pick_ref, back_ref, out_ref):
    devices, slots, piece = back_ref.shape
    rows = out_ref.shape[0]
    summed = jnp.dot(
        pick_ref[...], back_ref[...].reshape(devices * slots, piece), preferred_element_type=jnp.float32
    ).astype(jnp.bfloat16)
    for l in range(lanes_local):
        out_ref[:, l * piece : (l + 1) * piece] = summed[l * rows : (l + 1) * rows]


def on_device(tokens, expert_ids, gate_codes, gate_proj, up_proj, down_proj):
    nodes, locals_ = lax.axis_size("node"), lax.axis_size("local")
    own_rows, width = tokens.shape
    top = expert_ids.shape[1]
    slots = -(-(own_rows * NL) // nodes)
    devices = nodes * locals_
    half = width // 2
    total_rows = devices * slots
    send, pick = pl.pallas_call(
        functools.partial(dispatch_kernel, nodes, locals_, slots),
        out_shape=(
            jax.ShapeDtypeStruct((devices, slots, half + LANES), jnp.bfloat16),
            jax.ShapeDtypeStruct((locals_ * own_rows, total_rows), jnp.bfloat16),
        ),
        in_specs=[ANY] * 3,
        out_specs=(VMEM, VMEM),
        scratch_shapes=[
            pltpu.VMEM(tokens.shape, tokens.dtype),
            pltpu.VMEM(expert_ids.shape, expert_ids.dtype),
            pltpu.VMEM(gate_codes.shape, gate_codes.dtype),
            pltpu.SemaphoreType.DMA((3,)),
        ],
        compiler_params=small(4096),
        cost_estimate=pl.CostEstimate(flops=10**10, bytes_accessed=40 << 20, transcendentals=0),
        name="dispatch",
    )(*(pltpu.with_memory_space_constraint(a, pltpu.HBM) for a in (tokens, expert_ids, gate_codes)))
    arrived = lax.all_to_all(send, EVERY, split_axis=0, concat_axis=0, tiled=True)
    flip = lambda array, bit: lax.ppermute(array, "local", [(i, i ^ bit) for i in range(locals_)])
    other = flip(arrived, 1)

    per_lane = gate_proj.shape[1]
    sums = pl.pallas_call(
        functools.partial(first_kernel, half),
        out_shape=jax.ShapeDtypeStruct((total_rows, 2 * per_lane), jnp.float32),
        in_specs=[VMEM] + [pl.BlockSpec()] * 2,
        out_specs=VMEM,
        compiler_params=small(16384),
        name="first",
    )(arrived, gate_proj, up_proj)
    hidden = pl.pallas_call(
        functools.partial(second_kernel, half, top),
        out_shape=jax.ShapeDtypeStruct((total_rows, per_lane), jnp.bfloat16),
        in_specs=[VMEM] * 3 + [pl.BlockSpec()] * 2,
        out_specs=VMEM,
        compiler_params=small(16384),
        name="second",
    )(sums, arrived, other, gate_proj, up_proj)
    bits = [1 << b for b in range(1, locals_.bit_length() - 1)]
    far = {0: hidden}
    for bit in reversed(bits):
        far.update({key ^ bit: flip(piece, bit) for key, piece in list(far.items())})
    near_mask = (0, 1)
    near_pieces = (hidden, flip(hidden, 1))
    near = pl.pallas_call(
        functools.partial(down_near_kernel, near_mask),
        out_shape=jax.ShapeDtypeStruct((total_rows, down_proj.shape[1]), jnp.float32),
        in_specs=[VMEM] + [pl.BlockSpec()] * 2,
        out_specs=VMEM,
        compiler_params=small(16384),
        cost_estimate=pl.CostEstimate(flops=10**9, bytes_accessed=4 << 20, transcendentals=0),
        name="down_near",
    )(*near_pieces, down_proj)
    far.pop(0)
    keys = list(far)
    far_mask = tuple(keys) + tuple(key ^ 1 for key in keys)
    far_pieces = [far[key] for key in keys]
    far_pieces = far_pieces + [flip(piece, 1) for piece in far_pieces]
    contrib = pl.pallas_call(
        functools.partial(down_far_kernel, far_mask),
        out_shape=jax.ShapeDtypeStruct((devices, slots, down_proj.shape[1]), jnp.bfloat16),
        in_specs=[VMEM] * (len(far_mask) + 2),
        out_specs=VMEM,
        compiler_params=small(16384),
        name="down_far",
    )(*far_pieces, down_proj, near)
    back = lax.all_to_all(contrib, EVERY, split_axis=0, concat_axis=0, tiled=True)
    return pl.pallas_call(
        functools.partial(combine_kernel, locals_),
        out_shape=jax.ShapeDtypeStruct((own_rows, width), jnp.bfloat16),
        in_specs=[VMEM] * 2,
        out_specs=VMEM,
        compiler_params=small(4096),
        name="combine",
    )(pick, back)


def solution(mesh):
    return jax.shard_map(
        on_device,
        mesh=mesh,
        in_specs=(
            P(EVERY, None),
            P(EVERY, None),
            P(EVERY, None),
            P(None, EVERY),
            P(None, EVERY),
            P("node", "local"),
        ),
        out_specs=P(EVERY, None),
        check_vma=False,
    )
```

```python
import functools

import jax
import jax.numpy as jnp
from jax import lax
from jax.experimental import pallas as pl
from jax.experimental.pallas import tpu as pltpu
from jax.sharding import PartitionSpec as P


FF_E = 1024
EXP_NODE = 2
NL = 4
ROUTE_SCALE = 2.5
LANES = 128
CODE_BASE = 32
EVERY = ("node", "local")
HBM = pl.BlockSpec(memory_space=pltpu.HBM)
VMEM = pl.BlockSpec(memory_space=pltpu.VMEM)


def small(kib):
    return pltpu.CompilerParams(vmem_limit_bytes=kib << 10)


def split(index, size):
    whole = jnp.floor((index + 0.5) / size)
    return whole, index - whole * size


def slot_mask(ids, group, slot):
    lowest = group * EXP_NODE
    used = None
    for k in range(ids.shape[1]):
        offset = ids[:, k : k + 1] - lowest
        hit = (offset >= 0.0) & (offset < EXP_NODE)
        used = hit if used is None else used | hit
    used = jnp.where(used, 1.0, 0.0)
    ranks, so_far = [], jnp.zeros((1, group.shape[1]), jnp.float32)
    for t in range(ids.shape[0]):
        ranks.append(so_far)
        so_far = so_far + used[t : t + 1]
    return jnp.where(jnp.concatenate(ranks, axis=0) == slot, used, 0.0)


def pick_kernel(nodes, lanes_local, slots, ids_ref, pick_ref):
    ids = ids_ref[...].astype(jnp.float32)
    spot = lax.broadcasted_iota(jnp.int32, (ids.shape[0], nodes * lanes_local * slots), 1).astype(jnp.float32)
    device, slot = split(spot, slots)
    group, owner = split(device, lanes_local)
    mask = slot_mask(ids, group, slot)
    pick = [jnp.where(owner == l, mask, 0.0) for l in range(lanes_local)]
    pick_ref[...] = jnp.concatenate(pick, axis=0).astype(jnp.bfloat16)


def dispatch_kernel(nodes, lanes_local, slots, tok_hbm, ids_hbm, codes_hbm, out_ref, tok_ref, ids_ref, codes_ref, sems):
    copies = [
        pltpu.make_async_copy(source, target, sems.at[i])
        for i, (source, target) in enumerate(((ids_hbm, ids_ref), (codes_hbm, codes_ref), (tok_hbm, tok_ref)))
    ]
    for copy in copies:
        copy.start()
    copies[0].wait()
    rows, top = ids_ref.shape
    half = tok_ref.shape[1] // 2
    ids = ids_ref[...].astype(jnp.float32)
    spot = lax.broadcasted_iota(jnp.int32, (rows, nodes * slots), 1).astype(jnp.float32)
    mask = slot_mask(ids, *split(spot, slots)).astype(jnp.bfloat16)
    copies[1].wait()
    high, low = split(codes_ref[...].astype(jnp.float32), CODE_BASE)
    rest = jnp.zeros((rows, LANES - 3 * top), jnp.float32)
    score = jnp.concatenate([ids, high, low, rest], axis=1).astype(jnp.bfloat16)
    contract = (((0,), (0,)), ((), ()))
    scored = lax.dot_general(mask, score, contract, preferred_element_type=jnp.float32).astype(jnp.bfloat16)
    copies[2].wait()
    placed = lax.dot_general(mask, tok_ref[...], contract, preferred_element_type=jnp.float32).astype(jnp.bfloat16)
    for n in range(nodes):
        own = slice(n * slots, (n + 1) * slots)
        for l in range(lanes_local):
            side = l % 2
            out_ref[n * lanes_local + l, :, :half] = placed[own, side * half : (side + 1) * half]
            out_ref[n * lanes_local + l, :, half:] = scored[own]


def first_kernel(half, top, mine_ref, gate_ref, up_ref, sum_ref, scale_ref):
    local = lax.axis_index("local")
    part = pl.ds(pl.multiple_of(local % 2 * half, half), half)
    rows, width = sum_ref.shape[0], gate_ref.shape[1]
    mine = mine_ref[:, :, :half].reshape(rows, half)
    sum_ref[:, :width] = jnp.dot(mine, gate_ref[part, :], preferred_element_type=jnp.float32)
    sum_ref[:, width:] = jnp.dot(mine, up_ref[part, :], preferred_element_type=jnp.float32)
    expert = lax.axis_index("node") * EXP_NODE + local * width // FF_E
    score = mine_ref[:, :, half:].reshape(rows, LANES).astype(jnp.float32)
    codes = score[:, top : 2 * top] * CODE_BASE + score[:, 2 * top : 3 * top]
    named = jnp.where(score[:, :top] == expert.astype(jnp.float32), codes, 0.0)
    total = jnp.sum(codes, axis=1, keepdims=True)
    scale = ROUTE_SCALE * jnp.sum(named, axis=1, keepdims=True) / jnp.where(total > 0.0, total, 1.0)
    scale_ref[...] = jnp.broadcast_to(scale, scale_ref.shape)


def second_kernel(half, sum_ref, scale_ref, other_ref, gate_ref, up_ref, hidden_ref):
    local = lax.axis_index("local")
    part = pl.ds(pl.multiple_of((1 - local % 2) * half, half), half)
    rows, width = sum_ref.shape[0], gate_ref.shape[1]
    other = other_ref[:, :, :half].reshape(rows, half)
    if rows < LANES:
        other = jnp.concatenate([other, other], axis=0)
    pre_gate = jnp.dot(other, gate_ref[part, :], preferred_element_type=jnp.float32)
    pre_up = jnp.dot(other, up_ref[part, :], preferred_element_type=jnp.float32)
    pre_gate = sum_ref[:, :width] + pre_gate[:rows]
    pre_up = sum_ref[:, width:] + pre_up[:rows]
    scale = scale_ref[:, :1]
    hidden_ref[...] = (scale * (pre_gate / (1.0 + jnp.exp(-pre_gate))) * pre_up).astype(jnp.bfloat16)


def down_kernel(flips, adds, *refs):
    count = len(flips)
    pieces, down_ref, out_ref = refs[:count], refs[count], refs[-1]
    local = lax.axis_index("local")
    total = refs[count + 1][...] if adds else None
    for flip, piece in zip(flips, pieces):
        depth = piece.shape[1]
        part = pl.ds(pl.multiple_of((local ^ flip) * depth, depth), depth)
        term = jnp.dot(piece[...], down_ref[part, :], preferred_element_type=jnp.float32)
        total = term if total is None else total + term
    out_ref[...] = total.astype(out_ref.dtype).reshape(out_ref.shape)


def combine_kernel(lanes_local, pick_ref, back_ref, out_ref):
    devices, slots, piece = back_ref.shape
    rows = out_ref.shape[0]
    summed = jnp.dot(
        pick_ref[...], back_ref[...].reshape(devices * slots, piece), preferred_element_type=jnp.float32
    ).astype(jnp.bfloat16)
    for l in range(lanes_local):
        out_ref[:, l * piece : (l + 1) * piece] = summed[l * rows : (l + 1) * rows]


def hbm(*arrays):
    return tuple(pltpu.with_memory_space_constraint(array, pltpu.HBM) for array in arrays)


def layer(tokens, expert_ids, gate_codes, gate_proj, up_proj, down_proj):
    nodes, locals_ = lax.axis_size("node"), lax.axis_size("local")
    own_rows, width = tokens.shape
    top = expert_ids.shape[1]
    slots = -(-(own_rows * NL) // nodes)
    devices = nodes * locals_
    half = width // 2
    rows = devices * slots
    per_lane, out_width = gate_proj.shape[1], down_proj.shape[1]
    send = pl.pallas_call(
        functools.partial(dispatch_kernel, nodes, locals_, slots),
        out_shape=jax.ShapeDtypeStruct((devices, slots, half + LANES), jnp.bfloat16),
        in_specs=[HBM] * 3,
        out_specs=VMEM,
        scratch_shapes=[
            pltpu.VMEM(tokens.shape, tokens.dtype),
            pltpu.VMEM(expert_ids.shape, expert_ids.dtype),
            pltpu.VMEM(gate_codes.shape, gate_codes.dtype),
            pltpu.SemaphoreType.DMA((3,)),
        ],
        compiler_params=small(4096),
        cost_estimate=pl.CostEstimate(flops=10**10, bytes_accessed=40 << 20, transcendentals=0),
        name="dispatch",
    )(*hbm(tokens, expert_ids, gate_codes))
    arrived = lax.all_to_all(send, EVERY, split_axis=0, concat_axis=0, tiled=True)

    def flip(array, bit):
        return lax.ppermute(array, "local", [(i, i ^ bit) for i in range(locals_)])

    other = flip(arrived, 1)
    sums, scale = pl.pallas_call(
        functools.partial(first_kernel, half, top),
        out_shape=(
            jax.ShapeDtypeStruct((rows, 2 * per_lane), jnp.float32),
            jax.ShapeDtypeStruct((rows, LANES), jnp.float32),
        ),
        in_specs=[VMEM] + [pl.BlockSpec()] * 2,
        out_specs=(VMEM, VMEM),
        compiler_params=small(16384),
        name="first",
    )(arrived, gate_proj, up_proj)
    hidden = pl.pallas_call(
        functools.partial(second_kernel, half),
        out_shape=jax.ShapeDtypeStruct((rows, per_lane), jnp.bfloat16),
        in_specs=[VMEM] * 3 + [pl.BlockSpec()] * 2,
        out_specs=VMEM,
        compiler_params=small(16384),
        name="second",
    )(sums, scale, other, gate_proj, up_proj)

    def down(pieces, near=None, out=None):
        extra = () if near is None else (near,)
        return pl.pallas_call(
            functools.partial(down_kernel, tuple(pieces), near is not None),
            out_shape=out or jax.ShapeDtypeStruct((rows, out_width), jnp.float32),
            in_specs=[VMEM] * (len(pieces) + 1 + len(extra)),
            out_specs=VMEM,
            compiler_params=small(16384),
            cost_estimate=pl.CostEstimate(
                flops=2 * len(pieces) * rows * per_lane * out_width,
                bytes_accessed=2 * len(pieces) * per_lane * out_width,
                transcendentals=0,
            ),
        )(*pieces.values(), down_proj, *extra)

    far = {0: hidden}
    for b in reversed(range(1, locals_.bit_length() - 1)):
        for key, piece in list(far.items()):
            far[key ^ (1 << b)] = flip(piece, 1 << b)
    del far[0]
    near = down({0: hidden, 1: flip(hidden, 1)})
    relayed = {key ^ 1: flip(piece, 1) for key, piece in far.items()}
    pick = pl.pallas_call(
        functools.partial(pick_kernel, nodes, locals_, slots),
        out_shape=jax.ShapeDtypeStruct((locals_ * own_rows, rows), jnp.bfloat16),
        in_specs=[VMEM],
        out_specs=VMEM,
        compiler_params=small(4096),
        name="pick",
    )(expert_ids)
    lean = down(far, near)
    contrib = down(relayed, lean, jax.ShapeDtypeStruct((devices, slots, out_width), jnp.bfloat16))
    back = lax.all_to_all(contrib, EVERY, split_axis=0, concat_axis=0, tiled=True)
    return pl.pallas_call(
        functools.partial(combine_kernel, locals_),
        out_shape=jax.ShapeDtypeStruct((own_rows, width), jnp.bfloat16),
        in_specs=[VMEM] * 2,
        out_specs=VMEM,
        compiler_params=small(4096),
        name="combine",
    )(pick, back)


def solution(mesh):
    return jax.shard_map(
        layer,
        mesh=mesh,
        in_specs=(
            P(EVERY, None),
            P(EVERY, None),
            P(EVERY, None),
            P(None, EVERY),
            P(None, EVERY),
            P("node", "local"),
        ),
        out_specs=P(EVERY, None),
        check_vma=False,
    )
```

```python
import functools

import jax
import jax.numpy as jnp
from jax import lax
from jax.experimental import pallas as pl
from jax.experimental.pallas import tpu as pltpu
from jax.sharding import PartitionSpec as P


FF_E = 1024
EXP_NODE = 2
NL = 4
ROUTE_SCALE = 2.5
LANES = 128
CODE_BASE = 32
EVERY = ("node", "local")
HBM = pl.BlockSpec(memory_space=pltpu.HBM)
VMEM = pl.BlockSpec(memory_space=pltpu.VMEM)


def small(kib):
    return pltpu.CompilerParams(vmem_limit_bytes=kib << 10)


def split(index, size):
    whole = jnp.floor((index + 0.5) / size)
    return whole, index - whole * size


def slot_mask(ids, group, slot):
    lowest = group * EXP_NODE
    used = None
    for k in range(ids.shape[1]):
        offset = ids[:, k : k + 1] - lowest
        hit = (offset >= 0.0) & (offset < EXP_NODE)
        used = hit if used is None else used | hit
    used = jnp.where(used, 1.0, 0.0)
    ranks, so_far = [], jnp.zeros((1, group.shape[1]), jnp.float32)
    for t in range(ids.shape[0]):
        ranks.append(so_far)
        so_far = so_far + used[t : t + 1]
    return jnp.where(jnp.concatenate(ranks, axis=0) == slot, used, 0.0)


def pick_kernel(nodes, lanes_local, slots, ids_ref, pick_ref):
    ids = ids_ref[...].astype(jnp.float32)
    spot = lax.broadcasted_iota(jnp.int32, (ids.shape[0], nodes * lanes_local * slots), 1).astype(jnp.float32)
    device, slot = split(spot, slots)
    group, owner = split(device, lanes_local)
    mask = slot_mask(ids, group, slot)
    pick = [jnp.where(owner == l, mask, 0.0) for l in range(lanes_local)]
    pick_ref[...] = jnp.concatenate(pick, axis=0).astype(jnp.bfloat16)


def dispatch_kernel(nodes, lanes_local, slots, tok_hbm, ids_hbm, codes_hbm, out_ref, named_ref, tok_ref, ids_ref, codes_ref, sems):
    copies = [
        pltpu.make_async_copy(source, target, sems.at[i])
        for i, (source, target) in enumerate(((ids_hbm, ids_ref), (codes_hbm, codes_ref), (tok_hbm, tok_ref)))
    ]
    for copy in copies:
        copy.start()
    copies[0].wait()
    named_ref[...] = ids_ref[...]
    rows, top = ids_ref.shape
    half = tok_ref.shape[1] // 2
    ids = ids_ref[...].astype(jnp.float32)
    spot = lax.broadcasted_iota(jnp.int32, (rows, nodes * slots), 1).astype(jnp.float32)
    mask = slot_mask(ids, *split(spot, slots)).astype(jnp.bfloat16)
    copies[1].wait()
    high, low = split(codes_ref[...].astype(jnp.float32), CODE_BASE)
    rest = jnp.zeros((rows, LANES - 3 * top), jnp.float32)
    score = jnp.concatenate([ids, high, low, rest], axis=1).astype(jnp.bfloat16)
    contract = (((0,), (0,)), ((), ()))
    scored = lax.dot_general(mask, score, contract, preferred_element_type=jnp.float32).astype(jnp.bfloat16)
    copies[2].wait()
    placed = lax.dot_general(mask, tok_ref[...], contract, preferred_element_type=jnp.float32).astype(jnp.bfloat16)
    for n in range(nodes):
        own = slice(n * slots, (n + 1) * slots)
        for l in range(lanes_local):
            side = l % 2
            out_ref[n * lanes_local + l, :, :half] = placed[own, side * half : (side + 1) * half]
            out_ref[n * lanes_local + l, :, half:] = scored[own]


def first_kernel(half, top, mine_ref, gate_ref, up_ref, sum_ref, scale_ref):
    local = lax.axis_index("local")
    part = pl.ds(pl.multiple_of(local % 2 * half, half), half)
    rows, width = sum_ref.shape[0], gate_ref.shape[1]
    mine = mine_ref[:, :, :half].reshape(rows, half)
    sum_ref[:, :width] = jnp.dot(mine, gate_ref[part, :], preferred_element_type=jnp.float32)
    sum_ref[:, width:] = jnp.dot(mine, up_ref[part, :], preferred_element_type=jnp.float32)
    expert = lax.axis_index("node") * EXP_NODE + local * width // FF_E
    score = mine_ref[:, :, half:].reshape(rows, LANES).astype(jnp.float32)
    codes = score[:, top : 2 * top] * CODE_BASE + score[:, 2 * top : 3 * top]
    named = jnp.where(score[:, :top] == expert.astype(jnp.float32), codes, 0.0)
    total = jnp.sum(codes, axis=1, keepdims=True)
    scale = ROUTE_SCALE * jnp.sum(named, axis=1, keepdims=True) / jnp.where(total > 0.0, total, 1.0)
    scale_ref[...] = jnp.broadcast_to(scale, scale_ref.shape)


def second_kernel(half, sum_ref, scale_ref, other_ref, gate_ref, up_ref, hidden_ref):
    local = lax.axis_index("local")
    part = pl.ds(pl.multiple_of((1 - local % 2) * half, half), half)
    rows, width = sum_ref.shape[0], gate_ref.shape[1]
    other = other_ref[:, :, :half].reshape(rows, half)
    if rows < LANES:
        other = jnp.concatenate([other, other], axis=0)
    pre_gate = jnp.dot(other, gate_ref[part, :], preferred_element_type=jnp.float32)
    pre_up = jnp.dot(other, up_ref[part, :], preferred_element_type=jnp.float32)
    pre_gate = sum_ref[:, :width] + pre_gate[:rows]
    pre_up = sum_ref[:, width:] + pre_up[:rows]
    scale = scale_ref[:, :1]
    hidden_ref[...] = (scale * (pre_gate / (1.0 + jnp.exp(-pre_gate))) * pre_up).astype(jnp.bfloat16)


def down_kernel(flips, adds, *refs):
    count = len(flips)
    pieces, down_ref, out_ref = refs[:count], refs[count], refs[-1]
    local = lax.axis_index("local")
    total = refs[count + 1][...] if adds else None
    for flip, piece in zip(flips, pieces):
        depth = piece.shape[1]
        part = pl.ds(pl.multiple_of((local ^ flip) * depth, depth), depth)
        term = jnp.dot(piece[...], down_ref[part, :], preferred_element_type=jnp.float32)
        total = term if total is None else total + term
    out_ref[...] = total.astype(out_ref.dtype).reshape(out_ref.shape)


def combine_kernel(lanes_local, pick_ref, back_ref, out_ref):
    devices, slots, piece = back_ref.shape
    rows = out_ref.shape[0]
    summed = jnp.dot(
        pick_ref[...], back_ref[...].reshape(devices * slots, piece), preferred_element_type=jnp.float32
    ).astype(jnp.bfloat16)
    for l in range(lanes_local):
        out_ref[:, l * piece : (l + 1) * piece] = summed[l * rows : (l + 1) * rows]


def hbm(*arrays):
    return tuple(pltpu.with_memory_space_constraint(array, pltpu.HBM) for array in arrays)


def layer(tokens, expert_ids, gate_codes, gate_proj, up_proj, down_proj):
    nodes, locals_ = lax.axis_size("node"), lax.axis_size("local")
    own_rows, width = tokens.shape
    top = expert_ids.shape[1]
    slots = -(-(own_rows * NL) // nodes)
    devices = nodes * locals_
    half = width // 2
    rows = devices * slots
    per_lane, out_width = gate_proj.shape[1], down_proj.shape[1]
    send, named = pl.pallas_call(
        functools.partial(dispatch_kernel, nodes, locals_, slots),
        out_shape=(
            jax.ShapeDtypeStruct((devices, slots, half + LANES), jnp.bfloat16),
            jax.ShapeDtypeStruct(expert_ids.shape, expert_ids.dtype),
        ),
        in_specs=[HBM] * 3,
        out_specs=(VMEM, VMEM),
        scratch_shapes=[
            pltpu.VMEM(tokens.shape, tokens.dtype),
            pltpu.VMEM(expert_ids.shape, expert_ids.dtype),
            pltpu.VMEM(gate_codes.shape, gate_codes.dtype),
            pltpu.SemaphoreType.DMA((3,)),
        ],
        compiler_params=small(4096),
        name="dispatch",
    )(*hbm(tokens, expert_ids, gate_codes))
    pick = pl.pallas_call(
        functools.partial(pick_kernel, nodes, locals_, slots),
        out_shape=jax.ShapeDtypeStruct((locals_ * own_rows, rows), jnp.bfloat16),
        in_specs=[VMEM],
        out_specs=VMEM,
        compiler_params=small(4096),
        cost_estimate=pl.CostEstimate(flops=10**10, bytes_accessed=40 << 20, transcendentals=0),
        name="pick",
    )(named)
    send, pick = lax.optimization_barrier((send, pick))
    arrived = lax.all_to_all(send, EVERY, split_axis=0, concat_axis=0, tiled=True)

    def flip(array, bit):
        return lax.ppermute(array, "local", [(i, i ^ bit) for i in range(locals_)])

    other = flip(arrived, 1)
    sums, scale = pl.pallas_call(
        functools.partial(first_kernel, half, top),
        out_shape=(
            jax.ShapeDtypeStruct((rows, 2 * per_lane), jnp.float32),
            jax.ShapeDtypeStruct((rows, LANES), jnp.float32),
        ),
        in_specs=[VMEM] + [pl.BlockSpec()] * 2,
        out_specs=(VMEM, VMEM),
        compiler_params=small(16384),
        name="first",
    )(arrived, gate_proj, up_proj)
    hidden = pl.pallas_call(
        functools.partial(second_kernel, half),
        out_shape=jax.ShapeDtypeStruct((rows, per_lane), jnp.bfloat16),
        in_specs=[VMEM] * 3 + [pl.BlockSpec()] * 2,
        out_specs=VMEM,
        compiler_params=small(16384),
        name="second",
    )(sums, scale, other, gate_proj, up_proj)

    def down(pieces, near=None, out=None):
        extra = () if near is None else (near,)
        return pl.pallas_call(
            functools.partial(down_kernel, tuple(pieces), near is not None),
            out_shape=out or jax.ShapeDtypeStruct((rows, out_width), jnp.float32),
            in_specs=[VMEM] * (len(pieces) + 1 + len(extra)),
            out_specs=VMEM,
            compiler_params=small(16384),
            cost_estimate=pl.CostEstimate(
                flops=2 * len(pieces) * rows * per_lane * out_width,
                bytes_accessed=2 * len(pieces) * per_lane * out_width,
                transcendentals=0,
            ),
        )(*pieces.values(), down_proj, *extra)

    far = {0: hidden}
    for b in reversed(range(1, locals_.bit_length() - 1)):
        for key, piece in list(far.items()):
            far[key ^ (1 << b)] = flip(piece, 1 << b)
    del far[0]
    near = down({0: hidden, 1: flip(hidden, 1)})
    relayed = {key ^ 1: flip(hidden, key ^ 1) for key in far}
    lean = down(far, near)
    contrib = down(relayed, lean, jax.ShapeDtypeStruct((devices, slots, out_width), jnp.bfloat16))
    back = lax.all_to_all(contrib, EVERY, split_axis=0, concat_axis=0, tiled=True)
    return pl.pallas_call(
        functools.partial(combine_kernel, locals_),
        out_shape=jax.ShapeDtypeStruct((own_rows, width), jnp.bfloat16),
        in_specs=[VMEM] * 2,
        out_specs=VMEM,
        compiler_params=small(4096),
        name="combine",
    )(pick, back)


def solution(mesh):
    return jax.shard_map(
        layer,
        mesh=mesh,
        in_specs=(
            P(EVERY, None),
            P(EVERY, None),
            P(EVERY, None),
            P(None, EVERY),
            P(None, EVERY),
            P("node", "local"),
        ),
        out_specs=P(EVERY, None),
        check_vma=False,
    )
```
